128 devices in a mesh: pa: 8 (over z_lo, y), pb: 16 (over z_hi, x, core).
Axes of the slice: x: 4, y: 4, z: 4 (z_hi: 2, z_lo: 2; z = z_hi * 2 + z_lo), core: 2. Of those that a mesh axis runs over, the one named last changes fastest.
Arguments:
- right_side: float32 [128, 128, 256], P(None, 'pa', 'pb'), may hold values from -6 to 6
- coef_x: float32 [128, 128, 256], P(None, 'pa', 'pb'), may hold values from 0.1 to 4
- coef_y: float32 [128, 128, 256], P(None, 'pa', 'pb'), may hold values from 0.1 to 4
- coef_z: float32 [128, 128, 256], P(None, 'pa', 'pb'), may hold values from 0.1 to 4
Outputs:
- solution_field: float32 [128, 128, 256], P(None, 'pa', 'pb')
- residual: float32 [128, 128, 256], P(None, 'pa', 'pb')
The draws below stay inside these ranges and needn't reach their ends.
All inputs are finite; a program needn't handle non-finite values.
Results may differ from the reference program's by a relative error of at most 0.0003.
Values sent between devices are 32-bit elements.
A program may use at most 64 MiB of HBM per device.

```python
import math
import jax
import jax.numpy as jnp

ITERS = 4
NX = 128
NY = 128
NZ = 256


def block_scale(own_key, shape, shards, least, top_value):
    def one(axis_at, shards_of):
        steps = jax.random.uniform(jax.random.fold_in(jax.random.fold_in(own_key, 6), axis_at), (shards_of,), jnp.float32, least / len(shards), top_value / len(shards))
        return jnp.repeat(jnp.exp(steps), shape[axis_at] // shards_of).reshape((-1,) + (1,) * (len(shape) - axis_at - 1))

    gain = one(*shards[0])
    for cut in shards[1:]:
        gain = gain * one(*cut)
    return gain


def scatter_about(stream_key, extent, spread, bound, shards=(), held_as=jnp.bfloat16):
    loudness = block_scale(stream_key, extent, shards, -0.22, 0.18) if shards else 1.0
    entries = jax.random.normal(stream_key, extent, jnp.float32) * spread * loudness
    return jnp.minimum(jnp.maximum(entries, -bound), bound).astype(held_as)


def setup_inputs(seed: int = 0) -> dict:
    arg_keys = jax.random.split(jax.random.key(seed), 5)
    right_side = scatter_about(arg_keys[0], (NX, NY, NZ), 1.0, 6.0, ((1, 8), (2, 16)), jnp.float32)
    coef_x = jnp.clip(jnp.exp(math.log(4.0) - 3.6888794 * jax.random.uniform(arg_keys[1], (NX, NY, NZ), jnp.float32) ** block_scale(arg_keys[1], (NX, NY, NZ), ((1, 8), (2, 16)), -0.2, 0.2)), 0.1, 4.0)
    coef_y = jnp.clip(jnp.exp(math.log(4.0) - 3.6888794 * jax.random.uniform(arg_keys[2], (NX, NY, NZ), jnp.float32) ** block_scale(arg_keys[2], (NX, NY, NZ), ((1, 8), (2, 16)), -0.2, 0.2)), 0.1, 4.0)
    coef_z = jnp.clip(jnp.exp(math.log(4.0) - 3.6888794 * jax.random.uniform(arg_keys[3], (NX, NY, NZ), jnp.float32) ** block_scale(arg_keys[3], (NX, NY, NZ), ((1, 8), (2, 16)), -0.2, 0.2)), 0.1, 4.0)
    return {"right_side": right_side, "coef_x": coef_x, "coef_y": coef_y, "coef_z": coef_z}


mass_shift = 0.5
base_coef = 1.0


def wave_term(points):
    positions = jnp.arange(points).astype(jnp.float32)
    return 2.0 - 2.0 * jnp.cos(2.0 * jnp.pi * positions / points)


def precondition(grid_field):
    symbol = mass_shift + base_coef * (wave_term(NX)[:, None, None] + wave_term(NY)[None, :, None] + wave_term(NZ)[None, None, :])
    spectrum = jnp.fft.fftn(grid_field)
    return jnp.real(jnp.fft.ifftn(spectrum / symbol)).astype(jnp.float32)


def operate(grid_field, coef_x, coef_y, coef_z):
    result = mass_shift * grid_field
    for axis_number, weights in ((0, coef_x), (1, coef_y), (2, coef_z)):
        above_cells = jnp.roll(grid_field, -1, axis_number)
        below_cells = jnp.roll(grid_field, 1, axis_number)
        weights_low = jnp.roll(weights, 1, axis_number)
        result = result + weights * (grid_field - above_cells) + weights_low * (grid_field - below_cells)
    return result


def reference(right_side, coef_x, coef_y, coef_z):
    solution_field = jnp.zeros_like(right_side)
    residual = right_side
    precond = precondition(residual)
    direction = precond
    fit_now = jnp.sum(residual * precond)
    for iteration in range(ITERS):
        image_field = operate(direction, coef_x, coef_y, coef_z)
        step_size = fit_now / jnp.sum(direction * image_field)
        solution_field = solution_field + step_size * direction
        residual = residual - step_size * image_field
        if iteration + 1 < ITERS:
            precond = precondition(residual)
            fit_next = jnp.sum(residual * precond)
            direction = precond + (fit_next / fit_now) * direction
            fit_now = fit_next
    return solution_field, residual
```

```python
import functools

import jax
import jax.numpy as jnp
import numpy as np
from jax import lax
from jax.experimental import pallas as pl
from jax.experimental.pallas import tpu as pltpu
from jax.sharding import PartitionSpec as P

ITERS = 4
NA = 8
NB = 16
ND = NA * NB
MESH = pl.DeviceIdType.MESH
mass_shift = 0.5
base_coef = 1.0


def cas_matrix(points):
    index = np.arange(points)
    angle = 2.0 * np.pi * ((index[:, None] * index[None, :]) % points) / points
    return (np.cos(angle) + np.sin(angle)) / np.sqrt(points)


def split_constant(matrix):
    high = jnp.asarray(matrix, jnp.float32).astype(jnp.bfloat16)
    low = (jnp.asarray(matrix, jnp.float32) - high.astype(jnp.float32)).astype(jnp.bfloat16)
    return high, low


def wave(points):
    return 2.0 - 2.0 * np.cos(2.0 * np.pi * np.arange(points) / points)


def ring_distance(step):
    return min(step, 4 - step)


OFFSETS = [
    (dx, dy, dz, dc)
    for dx in range(4)
    for dy in range(4)
    for dz in range(4)
    for dc in range(2)
    if (dx, dy, dz, dc) != (0, 0, 0, 0)
]
OFFSETS.sort(
    key=lambda o: -(ring_distance(o[0]) + ring_distance(o[1]) + ring_distance(o[2]) + 0.5 * o[3])
)


def split(value):
    high = value.astype(jnp.bfloat16)
    low = (value - high.astype(jnp.float32)).astype(jnp.bfloat16)
    return high, low


def product(left, right, dims):
    def one(a, b):
        return lax.dot_general(a, b, (dims, ((), ())), preferred_element_type=jnp.float32)

    return one(left[0], right[0]) + (one(left[1], right[0]) + one(left[0], right[1]))


def lanes_to(value, index):
    return jnp.take_along_axis(value, index, axis=1)


def segment_transpose(value):
    rows = value.shape[0]
    row = lax.broadcasted_iota(jnp.int32, (8, 128), 0)
    lane = lax.broadcasted_iota(jnp.int32, (8, 128), 1)
    group, inner = lane // 16, lane % 16
    first = ((row + group) % 8) * 16 + inner
    middle = (row - group + 8) % 8
    last = ((row - group + 8) % 8) * 16 + inner
    done = []
    for start in range(0, rows, 8):
        tile = value[start : start + 8]
        tile = jnp.take_along_axis(tile, first, axis=1)
        tile = jnp.take_along_axis(tile, middle, axis=0)
        done.append(jnp.take_along_axis(tile, last, axis=1))
    return done


def kernel(
    b_ref, cx_ref, cy_ref, cz_ref, h1h_ref, h1l_ref, h2h_ref, h2l_ref, wy_ref, wz_ref,
    x_ref, r_ref,
    fs, fr, bs, br, lx_ref, ly_ref, lz_ref, diag_ref, zlast, ylow, zlow, inv_ref,
    rhat, shat, u_ref, w_ref, p_ref, s_ref, sc,
    f_send, f_recv, b_send, b_recv, e_sems,
):
    a = lax.axis_index("pa")
    b = lax.axis_index("pb")
    me = a * NB + b
    at_y, at_x, core = lax.rem(a, 4), lax.rem(b // 2, 4), lax.rem(b, 2)
    at_z = (b // 8) * 2 + a // 4
    part_x = [lax.rem(at_x + d, 4) * 2 for d in range(4)]
    part_y = [lax.rem(at_y + d, 4) for d in range(4)]
    part_za = [lax.rem(lax.rem(at_z + d, 4), 2) * 4 for d in range(4)]
    part_zb = [(lax.rem(at_z + d, 4) // 2) * 8 for d in range(4)]
    part_c = [core, 1 - core]

    def targets():
        for dx, dy, dz, dc in OFFSETS:
            yield part_za[dz] + part_y[dy], part_zb[dz] + part_x[dx] + part_c[dc]

    def exchange(source, target, send_sem, recv_sem):
        for ta, tb in targets():
            pltpu.make_async_remote_copy(
                source.at[ta * NB + tb], target.at[me], send_sem, recv_sem,
                device_id=(ta, tb), device_id_type=MESH,
            ).start()
        target[pl.ds(me, 1)] = source[pl.ds(me, 1)]

    def all_others(buffer, sem):
        part = buffer.at[pl.ds(0, ND - 1)]
        pltpu.make_async_copy(part, part, sem).wait()

    barrier = pltpu.get_barrier_semaphore()
    for ta, tb in targets():
        pl.semaphore_signal(barrier, inc=1, device_id=(ta, tb), device_id_type=MESH)

    h1 = (h1h_ref[...], h1l_ref[...])
    h2 = (h2h_ref[...], h2l_ref[...])

    def send_lines(field, partial):
        lines = product(h1, split(field), ((1,), (1,)))
        fs[:, 0, :] = lines[:, :128]
        fs[:, 1, :] = lines[:, 128:]
        fs[:, 2, :] = jnp.broadcast_to(partial, (ND, 128))
        exchange(fs, fr, f_send, f_recv)

    rhs = b_ref[...]
    zlast[...] = cz_ref[...].reshape(16, 16, 128)[:, 15, :]
    r_ref[...] = rhs
    zero = jnp.zeros((256, 128), jnp.float32)
    for ref in (x_ref, u_ref, w_ref, p_ref, s_ref):
        ref[...] = zero
    rhat[...] = jnp.zeros_like(rhat)
    shat[...] = jnp.zeros_like(shat)

    pl.semaphore_wait(barrier, ND - 1)
    send_lines(rhs, jnp.zeros((1, 128), jnp.float32))
    edge_y = pltpu.make_async_remote_copy(
        cy_ref.at[pl.ds(240, 16)], ylow, e_sems.at[0], e_sems.at[1],
        device_id=(lax.rem(a + 1, NA), b), device_id_type=MESH,
    )
    edge_z = pltpu.make_async_remote_copy(
        zlast, zlow, e_sems.at[2], e_sems.at[3],
        device_id=(a, lax.rem(b + 1, NB)), device_id_type=MESH,
    )
    edge_y.start()
    edge_z.start()

    symbol = mass_shift + base_coef * (
        wy_ref[pl.ds(me, 1), 0:1] + wy_ref[:, 0:1] + wz_ref[...]
    )
    inv_ref[...] = 1.0 / symbol

    def below_z(field, edge):
        cube = field.reshape(16, 16, 128)
        return jnp.concatenate([edge[:, None, :], cube[:, :15]], axis=1).reshape(256, 128)

    def above_z(field, edge):
        cube = field.reshape(16, 16, 128)
        return jnp.concatenate([cube[:, 1:], edge[:, None, :]], axis=1).reshape(256, 128)

    edge_y.wait()
    edge_z.wait()
    cx, cy, cz = cx_ref[...], cy_ref[...], cz_ref[...]
    lower_x = pltpu.roll(cx, 1, 1)
    lower_y = jnp.concatenate([ylow[...], cy[:240]], axis=0)
    lower_z = below_z(cz, zlow[...])
    lx_ref[...] = lower_x
    ly_ref[...] = lower_y
    lz_ref[...] = lower_z
    diag_ref[...] = mass_shift + ((cx + lower_x) + (cy + lower_y) + (cz + lower_z))

    lane = lax.broadcasted_iota(jnp.int32, (128, 128), 1)
    lane_row = lax.broadcasted_iota(jnp.int32, (1, 128), 1)
    low_half = jnp.where(
        lane < 32, lane % 16, jnp.where(lane < 48, (lane % 8) * 16 + 15, (lane % 8) * 16)
    )
    high_half = jnp.where(
        lane < 32, lane % 16 + 112, jnp.where(lane < 48, (lane % 8) * 16 + 15, (lane % 8) * 16)
    )
    from_high = (lane < 16) | ((lane >= 32) & (lane % 16 >= 8))

    def slab(step, beta):
        tiles = [segment_transpose(fr[:, half, :]) for half in range(2)]
        plane = jnp.concatenate(
            [
                jnp.concatenate(
                    [tiles[half][2 * row + part] for row in range(NA) for half in range(2)], axis=0
                )
                for part in range(2)
            ],
            axis=1,
        )
        freq = product(split(plane), h2, ((1,), (0,)))
        freq = product(h1, split(freq), ((1,), (0,)))
        new_s = freq + beta * shat[...]
        new_r = rhat[...] - step * new_s
        shat[...] = new_s
        rhat[...] = new_r
        scaled = new_r * inv_ref[...]
        part_fit = jnp.sum(new_r * scaled, keepdims=True)
        back = product(h1, split(scaled), ((1,), (0,)))
        back = product(split(back), h2, ((1,), (0,)))
        out = [segment_transpose(back[:, part * 128 : part * 128 + 128]) for part in range(2)]
        halves = [
            jnp.concatenate(
                [out[part][2 * row + half] for row in range(NA) for part in range(2)], axis=0
            )
            for half in range(2)
        ]
        edges = jnp.where(
            from_high, lanes_to(halves[1], high_half), lanes_to(halves[0], low_half)
        )
        cube = edges.reshape(NA, NB, 128)
        from_low_z = jnp.concatenate([cube[:, 15:], cube[:, :15]], axis=1).reshape(ND, 128)
        from_high_z = jnp.concatenate([cube[:, 1:], cube[:, :1]], axis=1).reshape(ND, 128)
        from_low_y = jnp.concatenate([edges[112:], edges[:112]], axis=0)
        from_high_y = jnp.concatenate([edges[16:], edges[:16]], axis=0)
        halo = jnp.where(
            lane < 32,
            jnp.where(lane < 16, from_low_y, from_high_y),
            jnp.where(lane < 48, from_low_z, from_high_z),
        )
        bs[:, 0, :] = halves[0]
        bs[:, 1, :] = halves[1]
        bs[:, 2, :] = jnp.where(lane < 64, halo, jnp.broadcast_to(part_fit, (ND, 128)))
        exchange(bs, br, b_send, b_recv)

    def scalars(turn, fit, fit_old, step_old, curvature):
        beta = jnp.where(turn <= 1, 0.0, fit / fit_old)
        step = fit / (curvature - jnp.where(turn <= 1, 0.0, beta * fit / step_old))
        return jnp.where(turn == 0, -1.0, step), beta

    def update(step, beta):
        new_p = u_ref[...] + beta * p_ref[...]
        new_s = w_ref[...] + beta * s_ref[...]
        p_ref[...] = new_p
        s_ref[...] = new_s
        x_ref[...] = x_ref[...] + step * new_p
        r_ref[...] = r_ref[...] - step * new_s

    def turn_body(turn, carry):
        fit, fit_old, step_old = sc[0:1], sc[1:2], sc[2:3]
        all_others(fr, f_recv)
        curvature = jnp.sum(fr[:, 2, :], axis=0, keepdims=True)
        step, beta = scalars(turn, fit, fit_old, step_old, curvature)
        slab(step[:, 0:1], beta[:, 0:1])
        update(step, beta)

        all_others(br, b_recv)
        total = jnp.sum(br[:, 2, :], axis=0, keepdims=True)
        new_fit = jnp.where(lane_row < 64, pltpu.roll(total, 64, 1), total)
        lines = [product(split(br[:, k, :]), h1, ((0,), (0,))) for k in range(3)]
        u = jnp.concatenate(lines[:2], axis=0)
        halo = lines[2]
        u_ref[...] = u
        image = diag_ref[...] * u
        image -= cx_ref[...] * pltpu.roll(u, 127, 1)
        image -= lx_ref[...] * pltpu.roll(u, 1, 1)
        image -= cy_ref[...] * jnp.concatenate([u[16:], halo[16:32]], axis=0)
        image -= ly_ref[...] * jnp.concatenate([halo[0:16], u[:240]], axis=0)
        image -= cz_ref[...] * above_z(u, halo[48:64])
        image -= lz_ref[...] * below_z(u, halo[32:48])
        w_ref[...] = image
        all_others(fs, f_send)
        send_lines(image, jnp.sum(u * image, keepdims=True))
        all_others(bs, b_send)
        sc[0:1] = new_fit
        sc[1:2] = fit
        sc[2:3] = step
        return carry

    sc[...] = jnp.ones_like(sc)
    lax.fori_loop(0, ITERS, turn_body, 0)
    fit, fit_old, step_old = sc[0:1], sc[1:2], sc[2:3]
    all_others(fr, f_recv)
    curvature = jnp.sum(fr[:, 2, :], axis=0, keepdims=True)
    step, beta = scalars(ITERS, fit, fit_old, step_old, curvature)
    update(step, beta)
    all_others(fs, f_send)


def body(right_side, coef_x, coef_y, coef_z):
    def lines(value):
        return value.transpose(1, 2, 0).reshape(256, 128)

    h1 = split_constant(cas_matrix(128))
    h2 = split_constant(cas_matrix(256))
    wave_y = jnp.asarray(np.broadcast_to(wave(128)[:, None], (128, 128)), jnp.float32)
    wave_z = jnp.asarray(wave(256)[None, :], jnp.float32)
    message = pltpu.VMEM((ND, 3, 128), jnp.float32)
    block = pltpu.VMEM((256, 128), jnp.float32)
    plane = pltpu.VMEM((128, 256), jnp.float32)
    edge = pltpu.VMEM((16, 128), jnp.float32)
    vmem = pl.BlockSpec(memory_space=pltpu.VMEM)
    x, r = pl.pallas_call(
        kernel,
        out_shape=[jax.ShapeDtypeStruct((256, 128), jnp.float32)] * 2,
        in_specs=[vmem] * 10,
        out_specs=[vmem] * 2,
        scratch_shapes=[message] * 4 + [block] * 4 + [edge] * 3 + [plane] * 3 + [block] * 4
        + [pltpu.VMEM((8, 128), jnp.float32)]
        + [pltpu.SemaphoreType.DMA] * 4 + [pltpu.SemaphoreType.DMA((4,))],
        compiler_params=pltpu.CompilerParams(collective_id=0, has_side_effects=True),
    )(
        lines(right_side), lines(coef_x), lines(coef_y), lines(coef_z),
        h1[0], h1[1], h2[0], h2[1], wave_y, wave_z,
    )

    def block_of(value):
        return value.reshape(16, 16, 128).transpose(2, 0, 1)

    return block_of(x), block_of(r)


def solution(mesh):
    spec = P(None, "pa", "pb")
    return jax.shard_map(
        body, mesh=mesh, in_specs=(spec,) * 4, out_specs=(spec,) * 2, check_vma=False
    )
```

```python
import functools

import jax
import jax.numpy as jnp
import numpy as np
from jax import lax
from jax.experimental import pallas as pl
from jax.experimental.pallas import tpu as pltpu
from jax.sharding import PartitionSpec as P

ITERS = 4
NA = 8
NB = 16
ND = NA * NB
MESH = pl.DeviceIdType.MESH
mass_shift = 0.5
base_coef = 1.0


def cas_matrix(points):
    index = np.arange(points)
    angle = 2.0 * np.pi * ((index[:, None] * index[None, :]) % points) / points
    return (np.cos(angle) + np.sin(angle)) / np.sqrt(points)


def split_constant(matrix):
    single = matrix.astype(np.float32)
    high = single.astype(jnp.bfloat16)
    low = (single - high.astype(np.float32)).astype(jnp.bfloat16)
    return high, low


def wave(points):
    return 2.0 - 2.0 * np.cos(2.0 * np.pi * np.arange(points) / points)


def ring_distance(step):
    return min(step, 4 - step)


OFFSETS = [
    (dx, dy, dz, dc)
    for dx in range(4)
    for dy in range(4)
    for dz in range(4)
    for dc in range(2)
    if (dx, dy, dz, dc) != (0, 0, 0, 0)
]
OFFSETS.sort(
    key=lambda o: -(ring_distance(o[0]) + ring_distance(o[1]) + ring_distance(o[2]) + 0.5 * o[3])
)


def split(value):
    high = value.astype(jnp.bfloat16)
    low = (value - high.astype(jnp.float32)).astype(jnp.bfloat16)
    return high, low


def dot(left, right, dims=((1,), (0,))):
    return lax.dot_general(left, right, (dims, ((), ())), preferred_element_type=jnp.float32)


def from_left(stacked, value):
    rows = stacked.shape[0] // 2
    parts = dot(stacked, jnp.concatenate(split(value), axis=0))
    return parts[:rows] + parts[rows:]


def from_right(value, high, low):
    rows = value.shape[0]
    top, bottom = split(value)
    parts = dot(jnp.concatenate([top, bottom], axis=0), high)
    return parts[:rows] + (parts[rows:] + dot(top, low))


def take(buffer, row):
    return buffer.reshape(ND * 4, 128)[pl.ds(row, ND, stride=4), :]


def put(buffer, row, value):
    buffer.reshape(ND * 4, 128)[pl.ds(row, ND, stride=4), :] = value


def lanes_to(value, index):
    return jnp.take_along_axis(value, index, axis=1)


def segment_transpose(value):
    rows = value.shape[0]
    row = lax.broadcasted_iota(jnp.int32, (8, 128), 0)
    lane = lax.broadcasted_iota(jnp.int32, (8, 128), 1)
    group, inner = lane // 16, lane % 16
    first = ((row + group) % 8) * 16 + inner
    middle = (row - group + 8) % 8
    last = ((row - group + 8) % 8) * 16 + inner
    done = []
    for start in range(0, rows, 8):
        tile = value[start : start + 8]
        tile = jnp.take_along_axis(tile, first, axis=1)
        tile = jnp.take_along_axis(tile, middle, axis=0)
        done.append(jnp.take_along_axis(tile, last, axis=1))
    return done


def kernel(
    b_hbm, cx_hbm, cy_hbm, cz_hbm, h1_hbm, h2h_hbm, h2l_hbm, wy_hbm, wz_hbm,
    x_ref, r_ref,
    b_ref, cx_raw, cy_raw, cz_raw, h1_ref, h2h_ref, h2l_ref, wy_ref, wz_ref,
    fs, fr, bs, br, ds, dr, zlast, ylow, zlow,
    cx_ref, cy_ref, cz_ref, lx_ref, ly_ref, lz_ref, diag_ref, inv_ref,
    rhat, shat, u_ref, w_ref, p_ref, s_ref, xs_ref, halo_ref, sc,
    f_send, f_recv, b_send, b_recv, d_send, d_recv, e_sems, in_sems,
):
    loads = [
        pltpu.make_async_copy(source, target, in_sems.at[k])
        for k, (source, target) in enumerate(
            (
                (b_hbm, b_ref), (h1_hbm, h1_ref), (cy_hbm, cy_raw),
                (cz_hbm, cz_raw), (wy_hbm, wy_ref), (wz_hbm, wz_ref), (cx_hbm, cx_raw),
                (h2h_hbm, h2h_ref), (h2l_hbm, h2l_ref),
            )
        )
    ]
    for load in loads:
        load.start()
    a = lax.axis_index("pa")
    b = lax.axis_index("pb")
    me = a * NB + b
    at_y, at_x, core = lax.rem(a, 4), lax.rem(b // 2, 4), lax.rem(b, 2)
    at_z = (b // 8) * 2 + a // 4
    part_x = [lax.rem(at_x + d, 4) * 2 for d in range(4)]
    part_y = [lax.rem(at_y + d, 4) for d in range(4)]
    part_za = [lax.rem(lax.rem(at_z + d, 4), 2) * 4 for d in range(4)]
    part_zb = [(lax.rem(at_z + d, 4) // 2) * 8 for d in range(4)]
    part_c = [core, 1 - core]

    def targets():
        for dx, dy, dz, dc in OFFSETS:
            yield part_za[dz] + part_y[dy], part_zb[dz] + part_x[dx] + part_c[dc]

    def send(source, target, send_sem, recv_sem, ta, tb):
        pltpu.make_async_remote_copy(
            source, target, send_sem, recv_sem, device_id=(ta, tb), device_id_type=MESH
        ).start()

    def exchange(source, target, send_sem, recv_sem):
        for ta, tb in targets():
            send(
                source.at[ta * NB + tb, pl.ds(0, 3)], target.at[me, pl.ds(0, 3)],
                send_sem, recv_sem, ta, tb,
            )
        target[pl.ds(me, 1)] = source[pl.ds(me, 1)]

    def all_others(buffer, sem):
        part = buffer.at[pl.ds(0, ND - 1), pl.ds(0, min(3, buffer.shape[1]))]
        pltpu.make_async_copy(part, part, sem).wait()

    barrier = pltpu.get_barrier_semaphore()
    for ta, tb in targets():
        pl.semaphore_signal(barrier, inc=1, device_id=(ta, tb), device_id_type=MESH)

    for load in loads[:2]:
        load.wait()
    h1 = h1_ref[...]

    def fill(lines, partial):
        put(fs, 0, lines[:, :128])
        put(fs, 1, lines[:, 128:])
        put(fs, 2, jnp.broadcast_to(partial, (ND, 128)))

    fill(from_left(h1, b_ref[...].T), jnp.zeros((1, 128), jnp.float32))
    loads[2].wait()
    loads[3].wait()
    zlast[...] = cz_raw[...].reshape(16, 16, 128)[:, 15, :]
    for ref in (u_ref, w_ref, p_ref, s_ref, xs_ref, rhat, shat):
        ref[...] = jnp.zeros_like(ref)
    sc[...] = jnp.ones_like(sc)

    pl.semaphore_wait(barrier, ND - 1)
    exchange(fs, fr, f_send, f_recv)
    edge_y = pltpu.make_async_remote_copy(
        cy_raw.at[pl.ds(240, 16)], ylow, e_sems.at[0], e_sems.at[1],
        device_id=(lax.rem(a + 1, NA), b), device_id_type=MESH,
    )
    edge_z = pltpu.make_async_remote_copy(
        zlast, zlow, e_sems.at[2], e_sems.at[3],
        device_id=(a, lax.rem(b + 1, NB)), device_id_type=MESH,
    )
    edge_y.start()
    edge_z.start()
    for load in loads[4:]:
        load.wait()

    symbol = mass_shift + base_coef * (
        wy_ref[pl.ds(me, 1), 0:1] + wy_ref[:, 0:1] + wz_ref[...]
    )
    inv_ref[...] = 1.0 / symbol
    cx, cy, cz = cx_raw[...].T, cy_raw[...].T, cz_raw[...].T
    lower_x = pltpu.roll(cx, 1, 0)
    cx_ref[...] = cx
    cy_ref[...] = cy
    cz_ref[...] = cz
    lx_ref[...] = lower_x
    edge_y.wait()
    edge_z.wait()
    lower_y = jnp.concatenate([ylow[...], cy_raw[:240]], axis=0).T
    cube = cz_raw[...].reshape(16, 16, 128)
    lower_z = jnp.concatenate([zlow[...][:, None, :], cube[:, :15]], axis=1).reshape(256, 128).T
    ly_ref[...] = lower_y
    lz_ref[...] = lower_z
    diag_ref[...] = mass_shift + ((cx + lower_x) + (cy + lower_y) + (cz + lower_z))

    lane = lax.broadcasted_iota(jnp.int32, (128, 128), 1)
    in_line = lane % 16
    low_half = jnp.where(
        lane >= 112, lane - 112, jnp.where(lane < 32, (lane % 8) * 16 + 15, (lane % 8) * 16)
    )
    high_half = jnp.where(
        lane < 16, lane + 112, jnp.where(lane < 32, (lane % 8) * 16 + 15, (lane % 8) * 16)
    )
    from_high = (lane < 16) | ((lane < 48) & (in_line >= 8))
    spread = [
        jnp.where(in_line == 0, 16, 32) + half * 8 + lane // 16 for half in range(2)
    ]

    def slab(step, beta):
        tiles = [segment_transpose(take(fr, half)) for half in range(2)]
        plane = jnp.concatenate(
            [
                jnp.concatenate(
                    [tiles[half][2 * row + part] for row in range(NA) for half in range(2)], axis=0
                )
                for part in range(2)
            ],
            axis=1,
        )
        freq = from_right(plane, h2h_ref[...], h2l_ref[...])
        freq = from_left(h1, freq)
        new_s = freq + beta * shat[...]
        new_r = rhat[...] - step * new_s
        shat[...] = new_s
        rhat[...] = new_r
        scaled = new_r * inv_ref[...]
        part_fit = jnp.sum(new_r * scaled, keepdims=True)
        back = from_left(h1, scaled)
        back = from_right(back, h2h_ref[...], h2l_ref[...])
        out = [segment_transpose(back[:, part * 128 : part * 128 + 128]) for part in range(2)]
        halves = [
            jnp.concatenate(
                [out[part][2 * row + half] for row in range(NA) for part in range(2)], axis=0
            )
            for half in range(2)
        ]
        edges = jnp.where(
            from_high, lanes_to(halves[1], high_half), lanes_to(halves[0], low_half)
        )
        cube = edges.reshape(NA, NB, 128)
        from_low_z = jnp.concatenate([cube[:, 15:], cube[:, :15]], axis=1).reshape(ND, 128)
        from_high_z = jnp.concatenate([cube[:, 1:], cube[:, :1]], axis=1).reshape(ND, 128)
        from_low_y = jnp.concatenate([edges[112:], edges[:112]], axis=0)
        from_high_y = jnp.concatenate([edges[16:], edges[:16]], axis=0)
        halo = jnp.where(
            lane < 48,
            jnp.where(lane < 16, from_low_y, jnp.where(lane < 32, from_low_z, from_high_z)),
            jnp.where(lane >= 112, from_high_y, jnp.broadcast_to(part_fit, (ND, 128))),
        )
        put(bs, 0, halves[0])
        put(bs, 1, halves[1])
        put(bs, 2, halo)
        exchange(bs, br, b_send, b_recv)

    def scalars(turn, curvature):
        fit, fit_old, step_old = sc[0:1], sc[1:2], sc[2:3]
        beta = jnp.where(turn <= 1, 0.0, fit / fit_old)
        step = fit / (curvature - jnp.where(turn <= 1, 0.0, beta * fit / step_old))
        return jnp.where(turn == 0, -1.0, step), beta

    def neighbours(u0, u1, halo):
        u = jnp.concatenate([u0, u1], axis=1)
        up = [pltpu.roll(v, 112, 1) for v in (u0, u1)]
        above_y = jnp.concatenate(
            [jnp.where(lane < 112, up[0], up[1]), jnp.where(lane < 112, up[1], halo)], axis=1
        )
        down = [pltpu.roll(v, 16, 1) for v in (u0, u1)]
        below_y = jnp.concatenate(
            [jnp.where(lane >= 16, down[0], halo), jnp.where(lane >= 16, down[1], down[0])], axis=1
        )
        ends = [lanes_to(halo, spread[half]) for half in range(2)]
        above_z = jnp.concatenate(
            [jnp.where(in_line < 15, pltpu.roll(v, 127, 1), e) for v, e in zip((u0, u1), ends)],
            axis=1,
        )
        below_z = jnp.concatenate(
            [jnp.where(in_line > 0, pltpu.roll(v, 1, 1), e) for v, e in zip((u0, u1), ends)],
            axis=1,
        )
        return pltpu.roll(u, 127, 0), pltpu.roll(u, 1, 0), above_y, below_y, above_z, below_z

    def turn_body(turn, carry):
        all_others(fr, f_recv)
        curvature = jnp.sum(take(fr, 2), axis=0, keepdims=True)
        step, beta = scalars(turn, curvature)
        slab(step[:, 0:1], beta[:, 0:1])
        new_p = u_ref[...] + beta[:, 0:1] * p_ref[...]
        new_s = w_ref[...] + beta[:, 0:1] * s_ref[...]
        p_ref[...] = new_p
        s_ref[...] = new_s
        xs_ref[...] = xs_ref[...] + step[:, 0:1] * new_p
        sc[1:2] = sc[0:1]
        sc[2:3] = step

        all_others(br, b_recv)
        total = jnp.sum(take(br, 2), axis=0, keepdims=True)
        sc[0:1] = jnp.broadcast_to(total[:, 64:65], (1, 128))
        u = from_left(h1, jnp.concatenate([take(br, k) for k in range(3)], axis=1))
        u0, u1, halo = u[:, :128], u[:, 128:256], u[:, 256:]
        u = u[:, :256]
        u_ref[...] = u
        above_x, below_x, above_y, below_y, above_z, below_z = neighbours(u0, u1, halo)
        halo_ref[...] = halo
        image = diag_ref[...] * u
        image -= cx_ref[...] * above_x
        image -= lx_ref[...] * below_x
        image -= cy_ref[...] * above_y
        image -= ly_ref[...] * below_y
        image -= cz_ref[...] * above_z
        image -= lz_ref[...] * below_z
        w_ref[...] = image
        partial = jnp.sum(u * image, keepdims=True)
        all_others(fs, f_send)

        @pl.when(turn < ITERS - 1)
        def _():
            fill(from_left(h1, w_ref[...]), partial)
            exchange(fs, fr, f_send, f_recv)

        @pl.when(turn == ITERS - 1)
        def _():
            ds[...] = jnp.broadcast_to(partial, (1, 128))
            for ta, tb in targets():
                send(ds, dr.at[me], d_send, d_recv, ta, tb)
            dr[pl.ds(me, 1)] = ds[...].reshape(1, 1, 128)

        all_others(bs, b_send)
        return carry

    lax.fori_loop(0, ITERS, turn_body, 0)
    beta = (sc[0:1] / sc[1:2])[:, 0:1]
    x_ref[...] = xs_ref[...].T
    u = u_ref[...]
    sides = neighbours(u[:, :128], u[:, 128:], halo_ref[...])
    total = (sides[0] + sides[1]) + (sides[2] + sides[3]) + (sides[4] + sides[5])
    r_ref[...] = ((mass_shift + 6.0 * base_coef) * u - base_coef * total).T
    last_p = (u_ref[...] + beta * p_ref[...]).T
    last_s = (w_ref[...] + beta * s_ref[...]).T
    all_others(dr, d_recv)
    curvature = jnp.sum(dr.reshape(ND, 128)[...], axis=0, keepdims=True)
    step, beta = scalars(ITERS, curvature)
    x_ref[...] = x_ref[...] + step * last_p
    r_ref[...] = r_ref[...] - step * last_s
    all_others(dr, d_send)


def body(right_side, coef_x, coef_y, coef_z):
    def lines(value):
        return value.transpose(1, 2, 0).reshape(256, 128)

    h1 = np.concatenate([np.tile(part, (1, 2)) for part in split_constant(cas_matrix(128))])
    h2 = split_constant(cas_matrix(256))
    wave_y = np.broadcast_to(wave(128)[:, None], (128, 128)).astype(np.float32)
    wave_z = wave(256)[None, :].astype(np.float32)
    args = (
        lines(right_side), lines(coef_x), lines(coef_y), lines(coef_z),
        *(jnp.asarray(v) for v in (h1, h2[0], h2[1], wave_y, wave_z)),
    )
    message = pltpu.VMEM((ND, 4, 128), jnp.float32)
    plane = pltpu.VMEM((128, 256), jnp.float32)
    row = pltpu.VMEM((1, 128), jnp.float32)
    edge = pltpu.VMEM((16, 128), jnp.float32)
    vmem = pl.BlockSpec(memory_space=pltpu.VMEM)
    x, r = pl.pallas_call(
        kernel,
        out_shape=[pltpu.VMEM((256, 128), jnp.float32)] * 2,
        in_specs=[pl.BlockSpec(memory_space=pl.ANY)] * 9,
        out_specs=[vmem] * 2,
        scratch_shapes=[pltpu.VMEM(v.shape, v.dtype) for v in args]
        + [message] * 4 + [row, pltpu.VMEM((ND, 1, 128), jnp.float32)] + [edge] * 3
        + [plane] * 15 + [pltpu.VMEM((128, 128), jnp.float32)] + [pltpu.VMEM((8, 128), jnp.float32)]
        + [pltpu.SemaphoreType.DMA] * 6
        + [pltpu.SemaphoreType.DMA((4,)), pltpu.SemaphoreType.DMA((9,))],
        compiler_params=pltpu.CompilerParams(collective_id=0, has_side_effects=True),
    )(*args)

    def block_of(value):
        return value.reshape(16, 16, 128).transpose(2, 0, 1)

    return block_of(x), block_of(r)


def solution(mesh):
    spec = P(None, "pa", "pb")
    return jax.shard_map(
        body, mesh=mesh, in_specs=(spec,) * 4, out_specs=(spec,) * 2, check_vma=False
    )
```
